32 devices in a mesh: dp: 16 (over z, y, x), mp: 2 (over core).
Axes of the slice: x: 2, y: 2, z: 4, core: 2. Of those that a mesh axis runs over, the one named last changes fastest.
Arguments:
- grad: bfloat16 [4, 1024, 8192], P(None, 'dp', 'mp'), may hold values from -6 to 6
- second_moment: float32 [4, 1024, 8192], P(None, 'dp', 'mp'), may hold values from 0.004 to 20, as said below
- left_root: bfloat16 [2, 16, 1024, 1024], P('mp', 'dp'), as said below
- right_root: bfloat16 [2, 16, 1024, 1024], P('mp', 'dp'), as said below
- owner_slot: int32 [2, 4, 4], replicated, may hold values from 0 to 15, as said below
Outputs:
- update: bfloat16 [4, 1024, 8192], P(None, 'dp', 'mp')
The draws below stay inside these ranges and needn't reach their ends.
Inputs may be any that keep to these rules, and one draw needn't show every extreme that they name: For each h, owner_slot[h] lists every dp index exactly once: each dp index owns one block of each h. `second_moment`: positive. `left_root`: each square is symmetric positive definite. `right_root`: each square is symmetric positive definite.
All inputs are finite; a program needn't handle non-finite values.
Results may differ from the reference program's by a relative error of at most 0.0049.
Values may be sent and summed in bfloat16 or wider, within the bound.
A program may use at most 64 MiB of HBM per device.

```python
import jax
import jax.numpy as jnp
from jax import lax

D = 8192
BS = 1024
RB = 4
DH = 4096
CBH = 4
N_DP = 16
N_MP = 2


def draw_second_moment(key, part):
    key_rows, key_cols, key_elem = jax.random.split(jax.random.fold_in(key, 7), 3)
    position = jnp.arange(BS, dtype=jnp.float32) / (BS - 1)
    row_scale = jnp.exp(jax.random.uniform(key_rows, (RB, BS, 1), jnp.float32, jnp.log(0.3), jnp.log(3.0)))
    col_scale = jnp.exp(jax.random.uniform(key_cols, (RB, 1, D), jnp.float32, jnp.log(0.3), jnp.log(3.0)))
    trend = 3.0 ** (-position)
    element = jnp.exp(jax.random.uniform(key_elem, (RB, BS, D), jnp.float32, jnp.log(0.5), jnp.log(2.0)))
    return row_scale * col_scale * element * trend[None, :, None]


def root_square(key):
    key_diag, key_noise = jax.random.split(key)
    noise = jax.random.normal(key_noise, (BS, BS), jnp.float32)
    diagonal = jnp.exp(jax.random.uniform(key_diag, (BS,), jnp.float32, jnp.log(0.5), jnp.log(2.0)))
    spread = 0.2 / jnp.sqrt(2.0 * BS)
    return (noise + noise.T) * spread + jnp.diag(diagonal)


def root_stack(key):
    count = N_MP * N_DP
    keys = jax.random.split(key, count)
    squares = lax.map(root_square, keys)
    return squares.reshape(N_MP, N_DP, BS, BS)


def draw_left_root(key, part):
    return root_stack(jax.random.fold_in(key, 11)).astype(jnp.bfloat16)


def draw_right_root(key, part):
    return root_stack(jax.random.fold_in(key, 23)).astype(jnp.bfloat16)


def draw_owner_slot(key, part):
    halves = []
    for half_idx in range(N_MP):
        key_owner = jax.random.fold_in(key, 101 + half_idx)
        owners = jax.random.permutation(key_owner, N_DP).astype(jnp.int32)
        halves.append(owners.reshape(RB, CBH))
    return jnp.stack(halves).astype(jnp.int32)


def levels(own_key, dims, cuts, low, high):
    level = 1.0
    for dim, blocks in cuts:
        heights = jax.random.uniform(jax.random.fold_in(jax.random.fold_in(own_key, 6), dim), (blocks,), jnp.float32, low / len(cuts), high / len(cuts))
        level = level * jnp.repeat(jnp.exp(heights), dims[dim] // blocks).reshape((-1,) + (1,) * (len(dims) - 1 - dim))
    return level


def gaussian(own_key, shape, width, most, pieces=(), kind=jnp.bfloat16):
    result = jax.random.normal(own_key, shape, jnp.float32) * width
    if len(pieces) > 0:
        result = levels(own_key, shape, pieces, -0.22, 0.18) * result
    return jnp.clip(result, min=-most, max=most).astype(kind)


def setup_inputs(seed: int = 0) -> dict:
    arg_keys = jax.random.split(jax.random.key(seed), 6)
    return {
        "grad": gaussian(arg_keys[0], (RB, BS, D), 1.0, 6.0, ((1, 16), (2, 2))),
        "second_moment": draw_second_moment(jax.random.fold_in(arg_keys[5], 71), 0),
        "left_root": draw_left_root(jax.random.fold_in(arg_keys[5], 71), 0),
        "right_root": draw_right_root(jax.random.fold_in(arg_keys[5], 71), 0),
        "owner_slot": draw_owner_slot(jax.random.fold_in(arg_keys[5], 71), 0),
    }


BETA_TWO = 0.99
ADAM_EPS = 1e-08
NORM_EPS = 1e-06

def reference(grad, second_moment, left_root, right_root, owner_slot):
    widened = grad.astype(jnp.float32)
    moment_new = BETA_TWO * second_moment + (1.0 - BETA_TWO) * widened * widened
    direction = widened / (jnp.sqrt(moment_new) + ADAM_EPS)
    squares = lax.optimization_barrier(jnp.sum((direction * direction).reshape(RB, BS, N_MP, CBH, BS), axis=(1, 4)))

    def single(index):
        half_idx = index // (RB * CBH)
        row_idx = index // CBH % RB
        col_idx = index % CBH
        start = (half_idx * DH + col_idx * BS).astype(jnp.int32)
        block = lax.dynamic_slice(grad, (row_idx.astype(jnp.int32), jnp.int32(0), start), (1, BS, BS))[0]
        slot = owner_slot[half_idx, row_idx, col_idx]
        left = left_root[half_idx, slot]
        right = right_root[half_idx, slot]
        mixed = jnp.dot(block, right, preferred_element_type=jnp.float32).astype(jnp.bfloat16)
        shaped = jnp.dot(left, mixed, preferred_element_type=jnp.float32)
        shaped_sq = jnp.sum(shaped * shaped)
        adam_sq = squares[row_idx, half_idx, col_idx]
        factor = jnp.sqrt((adam_sq + NORM_EPS) / (shaped_sq + NORM_EPS))
        return (shaped * factor).astype(jnp.bfloat16)
    results = lax.map(single, jnp.arange(N_MP * RB * CBH, dtype=jnp.int32))
    results = results.reshape(N_MP, RB, CBH, BS, BS).transpose(1, 3, 0, 2, 4)
    return results.reshape(RB, BS, D)
```

```python
import functools

import jax
import jax.numpy as jnp
from jax import lax
from jax.experimental import pallas as pl
from jax.experimental.pallas import tpu as pltpu
from jax.sharding import PartitionSpec as P

BETA_TWO = 0.99
ADAM_EPS = 1e-08
NORM_EPS = 1e-06

LANES = 128
GROUP_ROWS = 256


def xor(a, k, n):
    value, bit = 0, 1
    while bit < n:
        value = value + ((a // bit + k // bit) % 2) * bit
        bit *= 2
    return value


def exchange_kernel(
    n, block_of, grad_hbm, moment_hbm, left_hbm, right_hbm, back,
    grad, moment, left, right, staged, arrived, mixed, total, result,
    parts, parts_out, parts_in,
    local_sem, grad_sem, send_sem, recv_sem, part_send, part_recv, back_send, back_recv,
):
    rows = grad.shape[1]
    size = left.shape[0]
    col_blocks = grad_hbm.shape[2] // size
    groups = max(size // GROUP_ROWS, 1)
    group = n // groups
    group_rows = size // groups
    me = lax.axis_index("dp")
    my_group, my_place = me // group, me % group
    send_order = [g for g in reversed(range(groups)) if g >= groups // 2]
    send_order = sorted(send_order)
    late_order = [g for g in reversed(range(groups)) if g < groups // 2]
    take_order = [g for g in range(groups // 2)] + send_order[::-1]

    def base_of(g):
        return xor(my_group, g, groups) * group

    def partner(g, j):
        return base_of(g) + (my_place + j) % group

    def over(g, body):
        def step(j, carry):
            body(partner(g, j))
            return carry

        lax.fori_loop(1 if g == 0 else 0, group, step, 0)

    barrier = pltpu.get_barrier_semaphore()
    for g in range(groups):
        over(g, lambda d: pl.semaphore_signal(barrier, inc=1, device_id={"dp": d}))

    def grad_load(b):
        cols = pl.ds(pl.multiple_of((b % col_blocks) * size, size), size)
        return pltpu.make_async_copy(
            grad_hbm.at[b // col_blocks, :, cols], grad.at[b], grad_sem.at[b]
        )

    def grad_start(b, carry):
        grad_load(b).start()
        return carry

    def grad_wait(b, carry):
        grad_load(b).wait()
        return carry

    lax.fori_loop(0, n, grad_start, 0)
    loads = [
        pltpu.make_async_copy(src, dst, local_sem.at[i])
        for i, (src, dst) in enumerate(
            [(moment_hbm, moment), (right_hbm.at[0, 0], right), (left_hbm.at[0, 0], left)]
        )
    ]
    for load in loads:
        load.start()

    def own_rows(s):
        return grad[block_of[s]]

    def chunk_copy(d):
        return pltpu.make_async_remote_copy(
            src_ref=staged.at[d], dst_ref=arrived.at[me], send_sem=send_sem.at[d],
            recv_sem=recv_sem.at[me], device_id={"dp": d},
        )

    def chunk_from(s):
        return pltpu.make_async_remote_copy(
            src_ref=staged.at[s], dst_ref=arrived.at[s], send_sem=send_sem.at[s],
            recv_sem=recv_sem.at[s], device_id={"dp": s},
        )

    def part_copy(d):
        return pltpu.make_async_remote_copy(
            src_ref=parts_out.at[d], dst_ref=parts_in.at[me], send_sem=part_send.at[d],
            recv_sem=part_recv.at[me], device_id={"dp": d},
        )

    def part_from(s):
        return pltpu.make_async_remote_copy(
            src_ref=parts_out.at[s], dst_ref=parts_in.at[s], send_sem=part_send.at[s],
            recv_sem=part_recv.at[s], device_id={"dp": s},
        )

    def back_copy(d):
        return pltpu.make_async_remote_copy(
            src_ref=result.at[d], dst_ref=back.at[me], send_sem=back_send.at[d],
            recv_sem=back_recv.at[me], device_id={"dp": d},
        )

    def back_from(s):
        return pltpu.make_async_remote_copy(
            src_ref=result.at[s], dst_ref=back.at[s], send_sem=back_send.at[s],
            recv_sem=back_recv.at[s], device_id={"dp": s},
        )

    def stage(d):
        staged[d] = own_rows(d)

    lax.fori_loop(0, n, grad_wait, 0)
    for g in send_order:
        over(g, stage)
    pl.semaphore_wait(barrier, n - 1)
    for g in send_order:
        over(g, lambda d: chunk_copy(d).start())
    for g in late_order:
        over(g, stage)
    arrived[me] = own_rows(me)
    loads[0].wait()

    piece = 2 * LANES

    def adam(b, carry):
        r, c = b // col_blocks, b % col_blocks
        sums = jnp.zeros((1, piece), jnp.float32)
        for p in range(size // piece):
            cols = pl.ds(pl.multiple_of(c * size + p * piece, piece), piece)
            widened = grad[b, :, p * piece : (p + 1) * piece].astype(jnp.float32)
            moment_new = BETA_TWO * moment[r, :, cols] + (1.0 - BETA_TWO) * widened * widened
            direction = widened / (jnp.sqrt(moment_new) + ADAM_EPS)
            sums = sums + jnp.sum(direction * direction, axis=0, keepdims=True)
        parts[b] = sums[:, :LANES] + sums[:, LANES:]
        return carry

    lax.fori_loop(0, n, adam, 0)

    def stage_part(d):
        parts_out[d] = parts[block_of[d]]

    for g in range(groups):
        over(g, stage_part)
    parts_in[me] = parts[block_of[me]]
    for g in send_order + late_order:
        over(g, lambda d: part_copy(d).start())
    for g in late_order:
        over(g, lambda d: chunk_copy(d).start())
    loads[1].wait()
    loads[2].wait()

    col_tile = min(size, 256)
    row_tile = min(size, 256)
    squares = jnp.zeros((8, size), jnp.float32)
    for position, g in enumerate(take_order):
        over(g, lambda s: chunk_from(s).wait_recv())
        base = base_of(g)

        def mix(t, carry):
            block = arrived[pl.ds(base, group)]
            if rows % 16 != 0:
                block = block.astype(jnp.float32)
            block = block.reshape(group_rows, size).astype(jnp.bfloat16)
            cols = pl.ds(pl.multiple_of(t * col_tile, col_tile), col_tile)
            mixed[:, cols] = jnp.dot(
                block, right[:, cols], preferred_element_type=jnp.float32
            ).astype(jnp.bfloat16)
            return carry

        lax.fori_loop(0, size // col_tile, mix, 0)
        depth = pl.ds(pl.multiple_of(base * rows, group_rows), group_rows)
        last = position == groups - 1

        def shape(t, sums):
            tile = pl.ds(pl.multiple_of(t * row_tile, row_tile), row_tile)
            term = jnp.dot(left[tile, depth], mixed[...], preferred_element_type=jnp.float32)
            if position > 0:
                term = total[tile, :] + term
            total[tile, :] = term
            if last:
                sums = sums + jnp.sum((term * term).reshape(row_tile // 8, 8, size), axis=0)
            return sums

        squares = lax.fori_loop(0, size // row_tile, shape, squares)

    for g in range(groups):
        over(g, lambda s: part_from(s).wait_recv())
    shaped_sq = jnp.sum(jnp.sum(squares, axis=0, keepdims=True), axis=1, keepdims=True)
    adam_sq = jnp.sum(jnp.sum(parts_in[...], axis=0), axis=1, keepdims=True)
    factor = jnp.sqrt((adam_sq + NORM_EPS) / (shaped_sq + NORM_EPS))

    def finish(d):
        tile = pl.ds(pl.multiple_of(d * rows, rows), rows)
        result[d] = (total[tile, :] * factor).astype(jnp.bfloat16)

    for g in send_order + late_order:
        over(g, finish)
        over(g, lambda d: back_copy(d).start())
    finish(me)
    own = pltpu.make_async_copy(result.at[me], back.at[me], local_sem.at[0])
    own.start()
    for g in range(groups):
        over(g, lambda d: chunk_copy(d).wait_send())
        over(g, lambda d: part_copy(d).wait_send())
    own.wait()
    for g in range(groups):
        over(g, lambda d: back_copy(d).wait_send())
        over(g, lambda s: back_from(s).wait_recv())


def place_kernel(n, table, back, out, held, in_sem, out_sem):
    col_blocks = out.shape[2] // back.shape[2]
    size = back.shape[2]
    half = lax.axis_index("mp")

    def fetch(b):
        owner = table[half, b // col_blocks, b % col_blocks]
        return pltpu.make_async_copy(back.at[owner], held.at[b], in_sem.at[b])

    def put(b):
        cols = pl.ds(pl.multiple_of((b % col_blocks) * size, size), size)
        return pltpu.make_async_copy(held.at[b], out.at[b // col_blocks, :, cols], out_sem.at[b])

    def first(b, carry):
        fetch(b).start()
        return carry

    def second(b, carry):
        fetch(b).wait()
        put(b).start()
        return carry

    def third(b, carry):
        put(b).wait()
        return carry

    lax.fori_loop(0, n, first, 0)
    lax.fori_loop(0, n, second, 0)
    lax.fori_loop(0, n, third, 0)


def per_device(grad, second_moment, left_root, right_root, owner_slot):
    row_blocks, rows, half_cols = grad.shape
    size = left_root.shape[-1]
    n = lax.axis_size("dp")
    group_rows = size // max(size // GROUP_ROWS, 1)
    smem = pl.BlockSpec(memory_space=pltpu.SMEM)
    anywhere = pl.BlockSpec(memory_space=pl.ANY)
    chunks = (n, rows, size)
    table = lax.dynamic_index_in_dim(owner_slot, lax.axis_index("mp"), 0, keepdims=False).reshape(-1)
    ids = lax.iota(jnp.int32, n)
    matches = table[None, :] == ids[:, None]
    block_of = jnp.sum(jnp.where(matches, ids[None, :], 0), axis=1)
    back = pl.pallas_call(
        functools.partial(exchange_kernel, n),
        out_shape=jax.ShapeDtypeStruct(chunks, jnp.bfloat16),
        in_specs=[smem] + [anywhere] * 4,
        out_specs=anywhere,
        scratch_shapes=[
            pltpu.VMEM(chunks, grad.dtype),
            pltpu.VMEM(second_moment.shape, jnp.float32),
            pltpu.VMEM((size, size), jnp.bfloat16),
            pltpu.VMEM((size, size), jnp.bfloat16),
            pltpu.VMEM(chunks, jnp.bfloat16),
            pltpu.VMEM(chunks, jnp.bfloat16),
            pltpu.VMEM((group_rows, size), jnp.bfloat16),
            pltpu.VMEM((size, size), jnp.float32),
            pltpu.VMEM(chunks, jnp.bfloat16),
            pltpu.VMEM((n, 1, LANES), jnp.float32),
            pltpu.VMEM((n, 1, LANES), jnp.float32),
            pltpu.VMEM((n, 1, LANES), jnp.float32),
            pltpu.SemaphoreType.DMA((3,)),
            pltpu.SemaphoreType.DMA((n,)),
        ]
        + [pltpu.SemaphoreType.DMA((n,))] * 6,
        compiler_params=pltpu.CompilerParams(collective_id=0, has_side_effects=True),
    )(block_of, grad, second_moment, left_root, right_root)
    return pl.pallas_call(
        functools.partial(place_kernel, n),
        out_shape=jax.ShapeDtypeStruct(grad.shape, jnp.bfloat16),
        in_specs=[smem, anywhere],
        out_specs=anywhere,
        scratch_shapes=[
            pltpu.VMEM(chunks, jnp.bfloat16),
            pltpu.SemaphoreType.DMA((n,)),
            pltpu.SemaphoreType.DMA((n,)),
        ],
    )(owner_slot, back)


def solution(mesh):
    in_specs = (
        P(None, "dp", "mp"),
        P(None, "dp", "mp"),
        P("mp", "dp", None, None),
        P("mp", "dp", None, None),
        P(),
    )
    out_specs = P(None, "dp", "mp")
    return jax.shard_map(
        per_device, mesh=mesh, in_specs=in_specs, out_specs=out_specs, check_vma=False
    )
```

```python
import functools

import jax
import jax.numpy as jnp
from jax import lax
from jax.experimental import pallas as pl
from jax.experimental.pallas import tpu as pltpu
from jax.sharding import PartitionSpec as P

BETA_TWO = 0.99
ADAM_EPS = 1e-08
NORM_EPS = 1e-06

LANES = 128
GROUP_ROWS = 256
VMEM_LIMIT = 48 * 1024 * 1024
FIRST = [1]
CROSS = [2, 3]
REST = [0]
BACK = [1, 2, 3, 0]
SKEW = True


def xor(a, k, n):
    value, bit = 0, 1
    while bit < n:
        value = value + ((a // bit + k // bit) % 2) * bit
        bit *= 2
    return value


def exchange_kernel(
    n, block_of, grad_hbm, moment_hbm, left_hbm, right_hbm, back,
    grad, moment, left, right, staged, arrived, mixed, total, result,
    parts, parts_out, parts_in,
    local_sem, grad_sem, send_sem, recv_sem, part_send, part_recv, back_send, back_recv,
):
    rows = grad.shape[1]
    size = left.shape[0]
    col_blocks = grad_hbm.shape[2] // size
    groups = max(size // GROUP_ROWS, 1)
    group = n // groups
    group_rows = size // groups
    me = lax.axis_index("dp")
    half = lax.axis_index("mp")
    my_group, my_place = me // group, me % group
    take_order = [0, 1] + CROSS

    def base_of(g):
        return xor(my_group, g, groups) * group

    def partner(g, j):
        return base_of(g) + (my_place + j) % group

    def over(g, body):
        def step(j, carry):
            body(partner(g, j))
            return carry

        lax.fori_loop(1 if g == 0 else 0, group, step, 0)

    barrier = pltpu.get_barrier_semaphore()
    for g in range(groups):
        over(g, lambda d: pl.semaphore_signal(barrier, inc=1, device_id={"dp": d}))

    def grad_load(b):
        cols = pl.ds(pl.multiple_of((b % col_blocks) * size, size), size)
        return pltpu.make_async_copy(
            grad_hbm.at[b // col_blocks, :, cols], grad.at[b], grad_sem.at[b]
        )

    def grad_start(b, carry):
        grad_load(b).start()
        return carry

    def grad_wait(b, carry):
        grad_load(b).wait()
        return carry

    lax.fori_loop(0, n, grad_start, 0)
    loads = [
        pltpu.make_async_copy(src, dst, local_sem.at[i])
        for i, (src, dst) in enumerate(
            [(moment_hbm, moment), (right_hbm.at[0, 0], right), (left_hbm.at[0, 0], left)]
        )
    ]
    for load in loads:
        load.start()

    def own_rows(s):
        return grad[block_of[half, s]]

    def chunk_copy(d):
        return pltpu.make_async_remote_copy(
            src_ref=staged.at[d], dst_ref=arrived.at[me], send_sem=send_sem.at[d],
            recv_sem=recv_sem.at[me], device_id={"dp": d},
        )

    def chunk_from(s):
        return pltpu.make_async_remote_copy(
            src_ref=staged.at[s], dst_ref=arrived.at[s], send_sem=send_sem.at[s],
            recv_sem=recv_sem.at[s], device_id={"dp": s},
        )

    def part_copy(d):
        return pltpu.make_async_remote_copy(
            src_ref=parts_out.at[d], dst_ref=parts_in.at[me], send_sem=part_send.at[d],
            recv_sem=part_recv.at[me], device_id={"dp": d},
        )

    def part_from(s):
        return pltpu.make_async_remote_copy(
            src_ref=parts_out.at[s], dst_ref=parts_in.at[s], send_sem=part_send.at[s],
            recv_sem=part_recv.at[s], device_id={"dp": s},
        )

    def back_copy(d):
        return pltpu.make_async_remote_copy(
            src_ref=result.at[d], dst_ref=back.at[me], send_sem=back_send.at[d],
            recv_sem=back_recv.at[me], device_id={"dp": d},
        )

    def back_from(s):
        return pltpu.make_async_remote_copy(
            src_ref=result.at[s], dst_ref=back.at[s], send_sem=back_send.at[s],
            recv_sem=back_recv.at[s], device_id={"dp": s},
        )

    def stage(d):
        staged[d] = own_rows(d)

    def send(gs):
        for g in gs:
            over(g, lambda d: chunk_copy(d).start())

    lax.fori_loop(0, n, grad_wait, 0)
    for g in FIRST + CROSS + REST:
        over(g, stage)
    pl.semaphore_wait(barrier, n - 1)
    pl.when(half == 0)(lambda: send(CROSS))
    send(FIRST + REST)
    arrived[me] = own_rows(me)
    loads[0].wait()

    piece = 2 * LANES

    def adam(b, carry):
        r, c = b // col_blocks, b % col_blocks
        sums = jnp.zeros((1, piece), jnp.float32)
        for p in range(size // piece):
            cols = pl.ds(pl.multiple_of(c * size + p * piece, piece), piece)
            widened = grad[b, :, p * piece : (p + 1) * piece].astype(jnp.float32)
            moment_new = BETA_TWO * moment[r, :, cols] + (1.0 - BETA_TWO) * widened * widened
            direction = widened / (jnp.sqrt(moment_new) + ADAM_EPS)
            sums = sums + jnp.sum(direction * direction, axis=0, keepdims=True)
        parts[b] = sums[:, :LANES] + sums[:, LANES:]
        return carry

    lax.fori_loop(0, n, adam, 0)

    def stage_part(d):
        parts_out[d] = parts[block_of[half, d]]

    for g in range(groups):
        over(g, stage_part)
    parts_in[me] = parts[block_of[half, me]]
    for g in range(groups):
        over(g, lambda d: part_copy(d).start())
    loads[1].wait()
    loads[2].wait()

    col_tile = min(size, 256)
    row_tile = min(size, 256)
    squares = jnp.zeros((8, size), jnp.float32)
    for position, g in enumerate(take_order):
        if SKEW and g == CROSS[0]:
            pl.when(half != 0)(lambda: send(CROSS))
        over(g, lambda s: chunk_from(s).wait_recv())
        base = base_of(g)

        def mix(t, carry):
            block = arrived[pl.ds(base, group)]
            if rows % 16 != 0:
                block = block.astype(jnp.float32)
            block = block.reshape(group_rows, size).astype(jnp.bfloat16)
            cols = pl.ds(pl.multiple_of(t * col_tile, col_tile), col_tile)
            mixed[:, cols] = jnp.dot(
                block, right[:, cols], preferred_element_type=jnp.float32
            ).astype(jnp.bfloat16)
            return carry

        lax.fori_loop(0, size // col_tile, mix, 0)
        depth = pl.ds(pl.multiple_of(base * rows, group_rows), group_rows)
        last = position == groups - 1

        def shape(t, sums):
            tile = pl.ds(pl.multiple_of(t * row_tile, row_tile), row_tile)
            term = jnp.dot(left[tile, depth], mixed[...], preferred_element_type=jnp.float32)
            if position > 0:
                term = total[tile, :] + term
            total[tile, :] = term
            if last:
                sums = sums + jnp.sum((term * term).reshape(row_tile // 8, 8, size), axis=0)
            return sums

        squares = lax.fori_loop(0, size // row_tile, shape, squares)

    for g in range(groups):
        over(g, lambda s: part_from(s).wait_recv())
    shaped_sq = jnp.sum(jnp.sum(squares, axis=0, keepdims=True), axis=1, keepdims=True)
    adam_sq = jnp.sum(jnp.sum(parts_in[...], axis=0), axis=1, keepdims=True)
    factor = jnp.sqrt((adam_sq + NORM_EPS) / (shaped_sq + NORM_EPS))

    def finish(d):
        tile = pl.ds(pl.multiple_of(d * rows, rows), rows)
        result[d] = (total[tile, :] * factor).astype(jnp.bfloat16)

    for g in BACK:
        over(g, finish)
        over(g, lambda d: back_copy(d).start())
    tile = pl.ds(pl.multiple_of(me * rows, rows), rows)
    back[me] = (total[tile, :] * factor).astype(jnp.bfloat16)
    for g in range(groups):
        over(g, lambda d: chunk_copy(d).wait_send())
        over(g, lambda d: part_copy(d).wait_send())
    for g in range(groups):
        over(g, lambda d: back_copy(d).wait_send())
        over(g, lambda s: back_from(s).wait_recv())


def place_kernel(n, table, back, out, sem):
    size = back.shape[2]
    col_blocks = out.shape[2] // size
    half = lax.axis_index("mp")

    def put(b):
        owner = table[half, b // col_blocks, b % col_blocks]
        cols = pl.ds(pl.multiple_of((b % col_blocks) * size, size), size)
        return pltpu.make_async_copy(back.at[owner], out.at[b // col_blocks, :, cols], sem.at[b])

    def start(b, carry):
        put(b).start()
        return carry

    def wait(b, carry):
        put(b).wait()
        return carry

    lax.fori_loop(0, n, start, 0)
    lax.fori_loop(0, n, wait, 0)


def per_device(grad, second_moment, left_root, right_root, owner_slot):
    row_blocks, rows, half_cols = grad.shape
    size = left_root.shape[-1]
    n = lax.axis_size("dp")
    group_rows = size // max(size // GROUP_ROWS, 1)
    smem = pl.BlockSpec(memory_space=pltpu.SMEM)
    hbm = pl.BlockSpec(memory_space=pltpu.HBM)
    vmem = pl.BlockSpec(memory_space=pltpu.VMEM)
    chunks = (n, rows, size)
    col_blocks = owner_slot.shape[2]
    block_ids = lax.broadcasted_iota(jnp.int32, (1, 1) + owner_slot.shape[1:], 2) * col_blocks
    block_ids = block_ids + lax.broadcasted_iota(jnp.int32, (1, 1) + owner_slot.shape[1:], 3)
    matches = owner_slot[:, None] == lax.iota(jnp.int32, n)[None, :, None, None]
    block_of = jnp.sum(jnp.where(matches, block_ids, 0), axis=(2, 3))
    back = pl.pallas_call(
        functools.partial(exchange_kernel, n),
        out_shape=pltpu.VMEM(chunks, jnp.bfloat16),
        in_specs=[smem] + [hbm] * 4,
        out_specs=vmem,
        scratch_shapes=[
            pltpu.VMEM(chunks, grad.dtype),
            pltpu.VMEM(second_moment.shape, jnp.float32),
            pltpu.VMEM((size, size), jnp.bfloat16),
            pltpu.VMEM((size, size), jnp.bfloat16),
            pltpu.VMEM(chunks, jnp.bfloat16),
            pltpu.VMEM(chunks, jnp.bfloat16),
            pltpu.VMEM((group_rows, size), jnp.bfloat16),
            pltpu.VMEM((size, size), jnp.float32),
            pltpu.VMEM(chunks, jnp.bfloat16),
            pltpu.VMEM((n, 1, LANES), jnp.float32),
            pltpu.VMEM((n, 1, LANES), jnp.float32),
            pltpu.VMEM((n, 1, LANES), jnp.float32),
            pltpu.SemaphoreType.DMA((3,)),
            pltpu.SemaphoreType.DMA((n,)),
        ]
        + [pltpu.SemaphoreType.DMA((n,))] * 6,
        compiler_params=pltpu.CompilerParams(
            collective_id=0, has_side_effects=True, vmem_limit_bytes=VMEM_LIMIT
        ),
    )(block_of, grad, second_moment, left_root, right_root)
    return pl.pallas_call(
        functools.partial(place_kernel, n),
        out_shape=jax.ShapeDtypeStruct(grad.shape, jnp.bfloat16),
        in_specs=[smem, vmem],
        out_specs=hbm,
        scratch_shapes=[pltpu.SemaphoreType.DMA((n,))],
        compiler_params=pltpu.CompilerParams(vmem_limit_bytes=VMEM_LIMIT),
    )(owner_slot, back)


def solution(mesh):
    in_specs = (
        P(None, "dp", "mp"),
        P(None, "dp", "mp"),
        P("mp", "dp", None, None),
        P("mp", "dp", None, None),
        P(),
    )
    out_specs = P(None, "dp", "mp")
    return jax.shard_map(
        per_device, mesh=mesh, in_specs=in_specs, out_specs=out_specs, check_vma=False
    )
```
